32 devices in a mesh: gx: 4 (over z), gy: 2 (over x), gz: 4 (over y, core).
Axes of the slice: x: 2, y: 2, z: 4, core: 2. Of those that a mesh axis runs over, the one named last changes fastest.
Arguments:
- images: float32 [2, 64, 64, 512], P(None, 'gx', 'gy', 'gz'), may hold values from -6 to 6
- velocity: float32 [2, 3, 8, 8, 64], P(None, None, 'gx', None, 'gz'), may hold values from -2 to 2
Outputs:
- new_velocity: float32 [2, 3, 8, 8, 64], P(None, None, 'gx', None, 'gz')
- velocity_field: bfloat16 [2, 3, 64, 64, 512], P(None, None, 'gx', 'gy', 'gz')
The draws below stay inside these ranges and needn't reach their ends.
All inputs are finite; a program needn't handle non-finite values.
Results may differ from the reference program's by a relative error of at most 0.001.
Values sent between devices are 32-bit elements; how exact they have to be, the bound alone decides.
A program may use at most 64 MiB of HBM per device.

```python
import jax
import jax.numpy as jnp
from jax import lax

NX = 64
NY = 64
NZ = 512
LX = 8
LY = 8
LZ = 64


def block_scale(own_key, dims, shards, low, high):
    def one(position, parts):
        draws = jax.random.uniform(jax.random.fold_in(jax.random.fold_in(own_key, 6), position), (parts,), jnp.float32, low / len(shards), high / len(shards))
        return jnp.repeat(jnp.exp(draws), dims[position] // parts).reshape((-1,) + (1,) * (len(dims) - position - 1))

    factor_of = one(*shards[0])
    for cut in shards[1:]:
        factor_of = factor_of * one(*cut)
    return factor_of


def scatter_about(rng, shape, width, bound, shards=(), held_as=jnp.bfloat16):
    drawn = jax.random.normal(rng, shape, jnp.float32) * width
    if len(shards) > 0:
        drawn = block_scale(rng, shape, shards, -0.22, 0.18) * drawn
    return jnp.clip(drawn, min=-bound, max=bound).astype(held_as)


def setup_inputs(seed: int = 0) -> dict:
    key_of = jax.random.split(jax.random.key(seed), 3)
    images = scatter_about(key_of[0], (2, NX, NY, NZ), 1.0, 6.0, ((1, 4), (2, 2), (3, 4)), jnp.float32)
    velocity = scatter_about(key_of[1], (2, 3, LX, LY, LZ), 0.3, 2.0, ((2, 4), (4, 4)), jnp.float32)
    return {"images": images, "velocity": velocity}


epsilon_value = 1e-5
step_size = 0.5


def spline_weight(offset):
    magnitude = jnp.abs(offset)
    interior = 2.0 / 3.0 - magnitude * magnitude + 0.5 * magnitude * magnitude * magnitude
    outside = jnp.maximum(2.0 - magnitude, 0.0)
    outside = outside * outside * outside / 6.0
    return jnp.where(magnitude < 1.0, interior, outside)


def spline_table(voxels, points, first_point):
    positions = jnp.arange(voxels, dtype=jnp.float32)[:, None]
    centres = 8.0 * (jnp.arange(points, dtype=jnp.float32)[None, :] + first_point) + 3.5
    return spline_weight((positions - centres) / 8.0)


def window_sum(values, which_axis, keep_count):
    running = lax.slice_in_dim(values, 0, keep_count, axis=which_axis)
    for offset in range(1, 9):
        running = running + lax.slice_in_dim(values, offset, offset + keep_count, axis=which_axis)
    return running


def gradient(volume, count_x, count_y, count_z):
    along_x = volume[5:5 + count_x, 4:4 + count_y, 4:4 + count_z] - volume[3:3 + count_x, 4:4 + count_y, 4:4 + count_z]
    along_y = volume[4:4 + count_x, 5:5 + count_y, 4:4 + count_z] - volume[4:4 + count_x, 3:3 + count_y, 4:4 + count_z]
    along_z = volume[4:4 + count_x, 4:4 + count_y, 5:5 + count_z] - volume[4:4 + count_x, 4:4 + count_y, 3:3 + count_z]
    return 0.5 * jnp.stack([along_x, along_y, along_z])


def local_forces(padded):
    count_x = padded.shape[1] - 8
    count_y = padded.shape[2] - 8
    count_z = padded.shape[3] - 8
    fixed_side = padded[0]
    moving_side = padded[1]
    products = jnp.stack([fixed_side, moving_side, fixed_side * fixed_side, moving_side * moving_side, fixed_side * moving_side])
    window_sums = window_sum(window_sum(window_sum(products, 1, count_x), 2, count_y), 3, count_z)
    averages = window_sums / 729.0
    mean_fixed = averages[0]
    mean_moving = averages[1]
    var_fixed = averages[2] - mean_fixed * mean_fixed + epsilon_value
    var_moving = averages[3] - mean_moving * mean_moving + epsilon_value
    covariance = averages[4] - mean_fixed * mean_moving
    centre_fixed = fixed_side[4:4 + count_x, 4:4 + count_y, 4:4 + count_z] - mean_fixed
    centre_moving = moving_side[4:4 + count_x, 4:4 + count_y, 4:4 + count_z] - mean_moving
    factor = 2.0 * covariance / (var_fixed * var_moving)
    pull_fixed = factor * (centre_moving - covariance / var_fixed * centre_fixed)
    pull_moving = factor * (centre_fixed - covariance / var_moving * centre_moving)
    return jnp.stack([pull_fixed[None] * gradient(fixed_side, count_x, count_y, count_z),
                      pull_moving[None] * gradient(moving_side, count_x, count_y, count_z)])


def reference(images, velocity):
    highest = lax.Precision.HIGHEST
    padded = jnp.pad(images, ((0, 0), (4, 4), (4, 4), (4, 4)))
    table_x = spline_table(NX, LX, 0.0)
    table_y = spline_table(NY, LY, 0.0)
    table_z = spline_table(NZ, LZ, 0.0)
    slab_count = NX // 8
    slab_ids = jnp.arange(slab_count, dtype=jnp.int32)

    def project_slab(slab_index):
        slab_rows = lax.dynamic_slice_in_dim(padded, slab_index * 8, 16, 1)
        pushes = local_forces(slab_rows)
        along_z = jnp.einsum('hcxyz,zk->hcxyk', pushes, table_z, precision=highest)
        return jnp.einsum('hcxyk,yj->hcxjk', along_z, table_y, precision=highest)

    partial_value = lax.map(project_slab, slab_ids)
    partial_value = jnp.moveaxis(partial_value, 0, 2).reshape(2, 3, NX, LY, LZ)
    descent = jnp.einsum('hcxjk,xi->hcijk', partial_value, table_x, precision=highest)
    new_velocity = velocity + step_size * descent

    def evaluate_slab(slab_index):
        table_rows = lax.dynamic_slice_in_dim(table_x, slab_index * 8, 8, 0)
        along_x = jnp.einsum('hcijk,xi->hcxjk', new_velocity, table_rows, precision=highest)
        along_y = jnp.einsum('hcxjk,yj->hcxyk', along_x, table_y, precision=highest)
        return jnp.einsum('hcxyk,zk->hcxyz', along_y, table_z, precision=highest).astype(jnp.bfloat16)

    field_slabs = lax.map(evaluate_slab, slab_ids)
    velocity_field = jnp.moveaxis(field_slabs, 0, 2).reshape(2, 3, NX, NY, NZ)
    return new_velocity, velocity_field
```

```python
import functools

import jax
import jax.numpy as jnp
from jax import lax
from jax.experimental import pallas as pl
from jax.experimental.pallas import tpu as pltpu
from jax.sharding import PartitionSpec as P

epsilon_value = 1e-05
step_size = 0.5
RAD = 4
MESH = pl.DeviceIdType.MESH
HIGH = lax.Precision.HIGHEST


def beta(offset):
    magnitude = jnp.abs(offset)
    interior = 2.0 / 3.0 - magnitude * magnitude + 0.5 * magnitude * magnitude * magnitude
    outside = jnp.maximum(2.0 - magnitude, 0.0)
    outside = outside * outside * outside / 6.0
    return jnp.where(magnitude < 1.0, interior, outside)


def beta_static(t):
    m = abs(t)
    if m < 1.0:
        return 2.0 / 3.0 - m * m + 0.5 * m * m * m
    return max(2.0 - m, 0.0) ** 3 / 6.0


def iota(shape, dim):
    return lax.broadcasted_iota(jnp.int32, shape, dim)


def lane_groups(lanes, groups, size):
    group = jnp.zeros_like(lanes)
    for n in range(1, groups + 1):
        group = group + (lanes >= n * size).astype(jnp.int32)
    return group, lanes - group * size


def split2(x):
    high = x.astype(jnp.bfloat16)
    low = (x - high.astype(jnp.float32)).astype(jnp.bfloat16)
    return high, low


def split3(x):
    high = x.astype(jnp.bfloat16)
    rest = x - high.astype(jnp.float32)
    mid = rest.astype(jnp.bfloat16)
    low = (rest - mid.astype(jnp.float32)).astype(jnp.bfloat16)
    return high, mid, low


def dot32(a, b):
    return jnp.dot(a, b, preferred_element_type=jnp.float32)


def dot_ones(x, ones_twice):
    high, mid, low = split3(x)
    depth = x.shape[1]
    return dot32(jnp.concatenate([high, mid], axis=1), ones_twice) + dot32(low, ones_twice[:depth])


def dot_split(x, table):
    high, low = split2(x)
    t_high, t_low = split2(table)
    return dot32(
        jnp.concatenate([high, low], axis=1), jnp.concatenate([t_high, t_high], axis=0)
    ) + dot32(high, t_low)


def force_kernel(
    counts, img, vel, w_ref, nv_ref,
    vol, hz, pack, xs, t3, h5, acc, velp, ptile, zrecv, slots, canvas,
    halo_send, halo_recv, z_send, z_recv, p_send, p_recv,
):
    nx, ny, nz = counts
    gx, gy, gz = lax.axis_index("gx"), lax.axis_index("gy"), lax.axis_index("gz")
    _, cx, cy, cz = img.shape
    bx, by, bz = cx // 8, cy // 8, cz // 8
    ly = vel.shape[3]
    wx, wz = bx + 4, bz + 4
    rows = cy + 16
    f32 = jnp.float32

    def exists(index, count, d):
        if d == 0:
            return True
        return index + d < count if d > 0 else index + d >= 0

    def valid(o):
        ok = None
        for index, count, d in zip((gx, gy, gz), counts, o):
            if d != 0:
                here = exists(index, count, d)
                ok = here if ok is None else ok & here
        return ok

    span = (-1, 0, 1)
    offsets = [(a, b, c) for c in span for a in span for b in span if (a, b, c) != (0, 0, 0)]
    offsets.sort(key=lambda o: abs(o[2]))
    peers = [(a, b) for a in range(nx) for b in range(ny) if (a, b) != (0, 0)]

    barrier = pltpu.get_barrier_semaphore()

    def greet(px, py, pz):
        pl.semaphore_signal(
            barrier, inc=1, device_id={"gx": px, "gy": py, "gz": pz}, device_id_type=MESH
        )

    for a, b in peers:
        greet(lax.rem(gx + a, nx), lax.rem(gy + b, ny), gz)
    for o in offsets:
        if o[2] != 0:

            @pl.when(valid(o))
            def _(o=o):
                greet(gx + o[0], gy + o[1], gz + o[2])

    lane = iota((cy, cz), 1)
    cell = lane // RAD
    edge_low = jnp.zeros((cy, cz), f32)
    edge_high = jnp.zeros((cy, cz), f32)
    for g in range(2 * cx):
        v = img[g // cx, g % cx]
        low = pltpu.roll(v, RAD * g, 1) if g else v
        shift = (RAD * g + RAD) % cz
        high = pltpu.roll(v, shift, 1) if shift else v
        edge_low = jnp.where(cell == g, low, edge_low)
        edge_high = jnp.where(cell == g, high, edge_high)
    pack[0] = edge_low
    pack[1] = edge_high

    def sides(index, count):
        return jnp.int32(index > 0) + jnp.int32(index < count - 1)

    beside = (1 + sides(gx, nx)) * (1 + sides(gy, ny)) * sides(gz, nz)
    pl.semaphore_wait(barrier, len(peers) + beside)

    def halo_copy(n, o):
        dx, dy, dz = o
        src_y = {-1: pl.ds(0, 8), 0: pl.ds(0, cy), 1: pl.ds(cy - 8, 8)}[dy]
        dst_y = {-1: pl.ds(cy + 8, 8), 0: pl.ds(8, cy), 1: pl.ds(0, 8)}[dy]
        if dz == 0:
            src_x = {-1: pl.ds(0, RAD), 0: pl.ds(0, cx), 1: pl.ds(cx - RAD, RAD)}[dx]
            dst_x = {-1: pl.ds(cx + RAD, RAD), 0: pl.ds(RAD, cx), 1: pl.ds(0, RAD)}[dx]
            src = img.at[:, src_x, src_y, :]
            dst = vol.at[:, dst_x, dst_y, :]
        else:
            src = pack.at[(dz + 1) // 2, src_y, :]
            dst = hz.at[(1 - dz) // 2, 1 - dx, dst_y, :]
        return pltpu.make_async_remote_copy(
            src_ref=src,
            dst_ref=dst,
            send_sem=halo_send.at[n],
            recv_sem=halo_recv.at[n],
            device_id={"gx": gx + dx, "gy": gy + dy, "gz": gz + dz},
            device_id_type=MESH,
        )

    for n, o in enumerate(offsets):

        @pl.when(valid(o))
        def _(n=n, o=o):
            halo_copy(n, o).start()

    vol[:, RAD : RAD + cx, 8 : 8 + cy, :] = img[...]

    velocity_lane = iota((bz, cz), 1)
    velocity_row = iota((bz, cz), 0)
    take = (iota((8, ly), 1) == by * gy + iota((8, ly), 0) - 2) & (iota((8, ly), 0) >= 2)
    take = (take & (iota((8, ly), 0) < 2 + by)).astype(f32)
    for c in range(6):
        placed = jnp.zeros((ly, cz), f32)
        for i in range(bx):
            spot = (velocity_lane == velocity_row + (2 + i) * wz + 2).astype(f32)
            placed = placed + jnp.dot(
                vel[c // 3, c % 3, i], spot, precision=HIGH, preferred_element_type=f32
            )
        velp[c] = jnp.dot(take, placed, precision=HIGH, preferred_element_type=f32)
    acc[...] = jnp.zeros(acc.shape, f32)

    band = (jnp.abs(iota((cz, cz), 0) - iota((cz, cz), 1)) <= RAD).astype(f32)
    band = jnp.concatenate([band, band], axis=0).astype(jnp.bfloat16)

    def edge_matrix(side, part, image):
        row, col = iota((cz, cz), 0), iota((cz, cz), 1)
        row_x = (row // RAD) % cx + cx * (part - 1)
        dz = row % RAD
        col_x = col // (2 * RAD)
        place = col % (2 * RAD)
        near = (row // (RAD * cx) == image) & (jnp.abs(row_x - col_x) <= RAD)
        if side == 0:
            reach = (place >= RAD) & (place - RAD <= dz)
        else:
            reach = (place < RAD) & (place >= dz)
        return (near & reach).astype(f32)

    edges = []
    for image in range(2):
        whole = jnp.concatenate(
            [edge_matrix(s, p, image) for s in range(2) for p in range(3)], axis=0
        )
        edges.append(jnp.concatenate([whole, whole], axis=0).astype(jnp.bfloat16))

    for n, o in enumerate(offsets):
        back = tuple(-d for d in o)

        @pl.when(valid(back))
        def _(n=n, o=o):
            halo_copy(n, o).wait_recv()

    @pl.when(gx == 0)
    def _():
        vol[:, 0:RAD] = jnp.zeros((2, RAD, rows, cz), f32)
        hz[:, 0] = jnp.zeros((2, rows, cz), f32)

    @pl.when(gx == nx - 1)
    def _():
        vol[:, cx + RAD :] = jnp.zeros((2, RAD, rows, cz), f32)
        hz[:, 2] = jnp.zeros((2, rows, cz), f32)

    @pl.when(gy == 0)
    def _():
        vol[:, :, 0:8] = jnp.zeros((2, cx + 2 * RAD, 8, cz), f32)
        hz[:, :, 0:8] = jnp.zeros((2, 3, 8, cz), f32)

    @pl.when(gy == ny - 1)
    def _():
        vol[:, :, 8 + cy :] = jnp.zeros((2, cx + 2 * RAD, 8, cz), f32)
        hz[:, :, 8 + cy :] = jnp.zeros((2, 3, 8, cz), f32)

    @pl.when(gz == 0)
    def _():
        hz[0] = jnp.zeros((3, rows, cz), f32)

    @pl.when(gz == nz - 1)
    def _():
        hz[1] = jnp.zeros((3, rows, cz), f32)

    def window_rows(count):
        tall = cy + 8
        t3[0:count] = (
            xs[0:count, 4 : 4 + tall] + xs[0:count, 5 : 5 + tall] + xs[0:count, 6 : 6 + tall]
        )
        return t3[0:count, 0:cy] + t3[0:count, 3 : 3 + cy] + t3[0:count, 6 : 6 + cy]

    for s in range(2):
        for p in range(3):
            t = hz[s, p]
            n = s * 3 + p
            xs[n] = t
            xs[6 + n] = t * t
            xs[12 + n] = t * pltpu.roll(t, cz // 2, 1)
    sums = window_rows(18)
    kinds = jnp.concatenate(
        [
            jnp.concatenate([sums[kind * 6 + n] for n in range(6)], axis=1)
            for kind in range(3)
        ],
        axis=0,
    )
    fixed_edge = dot_ones(kinds, edges[0])
    moving_edge = dot_ones(kinds[0 : 2 * cy], edges[1])
    h5[0] = fixed_edge[0:cy]
    h5[1] = moving_edge[0:cy]
    h5[2] = fixed_edge[cy : 2 * cy]
    h5[3] = moving_edge[cy : 2 * cy]
    h5[4] = fixed_edge[2 * cy :]
    h5[5] = jnp.where(
        lane % RAD == RAD - 1, hz[0, 1, 8 : 8 + cy], pltpu.roll(hz[1, 1, 8 : 8 + cy], 2, 1)
    )

    step = 4
    steps = cx // step

    def group(g, carry):
        first = g * step
        fs = [vol[0, first + d] for d in range(step + 8)]
        ms = [vol[1, first + d] for d in range(step + 8)]
        for k in range(5):
            if k == 0:
                a = fs
            elif k == 1:
                a = ms
            elif k == 2:
                a = [f * f for f in fs]
            elif k == 3:
                a = [m * m for m in ms]
            else:
                a = [f * m for f, m in zip(fs, ms)]
            common = a[3] + a[4] + a[5] + (a[6] + a[7] + a[8])
            left2 = a[1] + a[2]
            right2 = a[9] + a[10]
            xs[k * step] = common + (left2 + a[0])
            xs[k * step + 1] = common + (left2 + a[9])
            xs[k * step + 2] = common + (right2 + a[2])
            xs[k * step + 3] = common + (right2 + a[11])
        flat = window_rows(5 * step).reshape(5 * step * cy, cz)
        sums = dot_ones(flat, band).reshape(5, step, cy, cz)
        inner = (lane < RAD) | (lane >= cz - RAD)
        pulls = []
        for s in range(step):
            x = first + s
            shift = lax.rem(2 * cz - RAD - 2 * RAD * x, cz)
            mean = []
            for k in range(5):
                extra = jnp.where(inner, pltpu.roll(h5[k], shift, 1), 0.0)
                mean.append((sums[k, s] + extra) * (1.0 / 729.0))
            m_f, m_m, q_f, q_m, q_fm = mean
            var_f = q_f - m_f * m_f + epsilon_value
            var_m = q_m - m_m * m_m + epsilon_value
            cov = q_fm - m_f * m_m
            slope_f = cov / var_f
            slope_m = cov / var_m
            factor = (2.0 * 0.5 * step_size) * slope_f / var_m
            own_f = vol[0, x + RAD, 8 : 8 + cy]
            own_m = vol[1, x + RAD, 8 : 8 + cy]
            cen_f = own_f - m_f
            cen_m = own_m - m_m
            pull = [factor * (cen_m - slope_f * cen_f), factor * (cen_f - slope_m * cen_m)]
            forces = []
            for h, own in ((0, own_f), (1, own_m)):
                along_x = (
                    vol[h, x + RAD + 1, 8 : 8 + cy] - vol[h, x + RAD - 1, 8 : 8 + cy]
                )
                along_y = vol[h, x + RAD, 9 : 9 + cy] - vol[h, x + RAD, 7 : 7 + cy]
                turn = lax.rem(2 * cz - 3 - RAD * (h * cx + x), cz)
                beyond = pltpu.roll(h5[5], turn, 1)
                above = jnp.where(lane == cz - 1, beyond, pltpu.roll(own, cz - 1, 1))
                below = jnp.where(lane == 0, beyond, pltpu.roll(own, 1, 1))
                forces += [pull[h] * along_x, pull[h] * along_y, pull[h] * (above - below)]
            pulls.append(forces)
        half = lax.rem(g, 2)
        base = g // 2 + half
        for t in range(4):
            weights = []
            for s in range(step):
                low = beta_static(2 - t + (s - 3.5) / 8.0)
                high = beta_static(1 - t + (s + 4 - 3.5) / 8.0)
                weights.append(jnp.where(half == 0, f32(low), f32(high)))
            for c in range(6):
                total = pulls[0][c] * weights[0]
                for s in range(1, step):
                    total = total + pulls[s][c] * weights[s]
                acc[c, base + t] = acc[c, base + t] + total
        return carry

    lax.fori_loop(0, steps, group, 0)

    points_lane = iota((cz, cz), 1)
    _, table_k = lane_groups(points_lane, wx, wz)
    position = iota((cz, cz), 0) - 8 * (table_k - 2)
    table_z = beta((position.astype(f32) - 3.5) / 8.0)
    along = dot_split(acc[...].reshape(6 * wx * cy, cz), table_z).reshape(6, wx, cy, cz)
    lane_i, _ = lane_groups(lane, wx, wz)
    row_j = iota((8, cy), 0)
    table_y = beta((iota((8, cy), 1) - 8 * (row_j - 2)).astype(f32) / 8.0 - 3.5 / 8.0)
    table_y = table_y[: by + 4]
    for c in range(6):
        packed = jnp.zeros((cy, cz), f32)
        for i in range(wx):
            packed = jnp.where(lane_i == i, along[c, i], packed)
        ptile[c] = velp[c] + jnp.dot(
            table_y, packed, precision=HIGH, preferred_element_type=f32
        )

    def z_copy(n):
        d = 1 - 2 * n
        return pltpu.make_async_remote_copy(
            src_ref=ptile,
            dst_ref=zrecv.at[n],
            send_sem=z_send.at[n],
            recv_sem=z_recv.at[n],
            device_id={"gx": gx, "gy": gy, "gz": gz + d},
            device_id_type=MESH,
        )

    for n in range(2):

        @pl.when(exists(gz, nz, 1 - 2 * n))
        def _(n=n):
            z_copy(n).start()

    for n in range(2):
        here = exists(gz, nz, 2 * n - 1)

        @pl.when(here)
        def _(n=n):
            z_copy(n).wait_recv()

        @pl.when(jnp.logical_not(here))
        def _(n=n):
            zrecv[n] = jnp.zeros(ptile.shape, f32)

    tile_rows = 6 * (by + 4)
    tile_lane = iota((tile_rows, cz), 1)
    _, tile_k = lane_groups(tile_lane, wx, wz)
    from_left = pltpu.roll(zrecv[0].reshape(tile_rows, cz), cz - bz, 1)
    from_right = pltpu.roll(zrecv[1].reshape(tile_rows, cz), bz, 1)
    joined = (
        ptile[...].reshape(tile_rows, cz)
        + jnp.where(tile_k < 4, from_left, 0.0)
        + jnp.where(tile_k >= bz, from_right, 0.0)
    )
    me = gx * ny + gy
    slots[me] = joined.reshape(ptile.shape)

    def p_copy(n, a, b):
        return pltpu.make_async_remote_copy(
            src_ref=slots.at[me],
            dst_ref=slots.at[me],
            send_sem=p_send.at[n],
            recv_sem=p_recv.at[n],
            device_id={"gx": lax.rem(gx + a, nx), "gy": lax.rem(gy + b, ny), "gz": gz},
            device_id_type=MESH,
        )

    for n, (a, b) in enumerate(peers):
        p_copy(n, a, b).start()
    canvas[...] = jnp.zeros(canvas.shape, f32)
    for n, (a, b) in enumerate(peers):
        p_copy(n, a, b).wait_recv()

    for a in range(nx):
        for b in range(ny):
            spot = (a, slice(None), slice(by * b, by * b + by + 4))
            canvas[spot] = canvas[spot] + slots[a * ny + b]
    tall = canvas.shape[2]
    flat_lane = iota((6 * tall, cz), 1)
    full = jnp.zeros((6 * tall, cz), f32)
    for a in range(nx):
        move = bx * wz * (a - gx)
        part = pltpu.roll(canvas[a].reshape(6 * tall, cz), lax.rem(move + nx * cz, cz), 1)
        source = flat_lane - move
        full = full + jnp.where((source >= 0) & (source < wx * wz), part, 0.0)
    point_i, point_k = lane_groups(flat_lane, wx, wz)
    global_i = bx * gx - 2 + point_i
    global_k = bz * gz - 2 + point_k
    inside = (flat_lane < wx * wz) & (global_i >= 0) & (global_i < bx * nx)
    inside = inside & (global_k >= 0) & (global_k < bz * nz)
    full = jnp.where(inside, full, 0.0).reshape(6, tall, cz)
    row = iota((6, tall, cz), 1)
    full = jnp.where((row >= 2) & (row < 2 + ly), full, 0.0)
    canvas[0] = full
    for c in range(6):
        for i in range(bx):
            moved = pltpu.roll(canvas[0, c], cz - ((2 + i) * wz + 2), 1)
            nv_ref[c // 3, c % 3, i] = moved[2 : 2 + ly, 0:bz]
    window = canvas[0, :, 0 : by + 4]
    for b in range(1, ny):
        window = jnp.where(gy == b, canvas[0, :, by * b : by * b + by + 4], window)
    w_ref[...] = window

    for n, o in enumerate(offsets):

        @pl.when(valid(o))
        def _(n=n, o=o):
            halo_copy(n, o).wait_send()

    for n in range(2):

        @pl.when(exists(gz, nz, 1 - 2 * n))
        def _(n=n):
            z_copy(n).wait_send()

    for n, (a, b) in enumerate(peers):
        p_copy(n, a, b).wait_send()


def field_kernel(w_ref, out_ref, spread):
    cx, cy, cz = out_ref.shape[2:]
    bx, by, bz = cx // 8, cy // 8, cz // 8
    wx, wz = bx + 4, bz + 4
    wy = by + 4
    f32 = jnp.float32
    row = iota((cz, cz), 0)
    group, place = lane_groups(row, wx, wz)
    table = beta(((iota((cz, cz), 1) - 8 * (place - 2)).astype(f32) - 3.5) / 8.0)
    flat = w_ref[...].reshape(6 * wy, cz)
    lane_i, _ = lane_groups(iota((6 * wy, cz), 1), wx, wz)
    stack = jnp.concatenate([jnp.where(lane_i == i, flat, 0.0) for i in range(wx)], axis=0)
    spread[...] = dot_split(stack, table).reshape(wx, 6, wy, cz)
    sub = (iota((8, cz), 0).astype(f32) - 3.5) / 8.0
    taps = [beta(2.0 - t + sub) for t in range(5)]
    for c in range(6):
        for b in range(by):
            lines = []
            for i in range(wx):
                total = None
                for t in range(5):
                    term = taps[t] * spread[i, c, b + t : b + t + 1]
                    total = term if total is None else total + term
                lines.append(total)
            for x in range(cx):
                block, s = x // 8, x % 8
                half = s // 4
                total = None
                for t in range(half, half + 4):
                    term = beta_static(2 - t + (s - 3.5) / 8.0) * lines[block + t]
                    total = term if total is None else total + term
                out_ref[c // 3, c % 3, x, 8 * b : 8 * b + 8] = total.astype(jnp.bfloat16)


def shards(counts, images, velocity):
    nx, ny, nz = counts
    _, cx, cy, cz = images.shape
    bx, by, bz = cx // 8, cy // 8, cz // 8
    wy = by + 4
    tall = -(-(by * ny + 4) // 8) * 8
    rows = cy + 16
    f32 = jnp.float32
    vmem = pl.BlockSpec(memory_space=pltpu.VMEM)
    offsets = 26
    peers = nx * ny - 1
    window, new_velocity = pl.pallas_call(
        functools.partial(force_kernel, counts),
        out_shape=(
            jax.ShapeDtypeStruct((6, wy, cz), f32),
            jax.ShapeDtypeStruct(velocity.shape, f32),
        ),
        in_specs=[vmem, vmem],
        out_specs=(vmem, vmem),
        scratch_shapes=[
            pltpu.VMEM((2, cx + 2 * RAD, rows, cz), f32),
            pltpu.VMEM((2, 3, rows, cz), f32),
            pltpu.VMEM((2, cy, cz), f32),
            pltpu.VMEM((20, rows, cz), f32),
            pltpu.VMEM((20, cy + 8, cz), f32),
            pltpu.VMEM((6, cy, cz), f32),
            pltpu.VMEM((6, bx + 4, cy, cz), f32),
            pltpu.VMEM((6, wy, cz), f32),
            pltpu.VMEM((6, wy, cz), f32),
            pltpu.VMEM((2, 6, wy, cz), f32),
            pltpu.VMEM((nx * ny, 6, wy, cz), f32),
            pltpu.VMEM((nx, 6, tall, cz), f32),
            pltpu.SemaphoreType.DMA((offsets,)),
            pltpu.SemaphoreType.DMA((offsets,)),
            pltpu.SemaphoreType.DMA((2,)),
            pltpu.SemaphoreType.DMA((2,)),
            pltpu.SemaphoreType.DMA((peers,)),
            pltpu.SemaphoreType.DMA((peers,)),
        ],
        compiler_params=pltpu.CompilerParams(collective_id=0, has_side_effects=True),
        name="forces",
    )(images, velocity)
    field = pl.pallas_call(
        field_kernel,
        out_shape=jax.ShapeDtypeStruct((2, 3, cx, cy, cz), jnp.bfloat16),
        in_specs=[vmem],
        out_specs=vmem,
        scratch_shapes=[pltpu.VMEM((bx + 4, 6, wy, cz), f32)],
        name="field",
    )(window)
    return new_velocity, field


def solution(mesh):
    placed = (P(None, "gx", "gy", "gz"), P(None, None, "gx", None, "gz"))
    counts = tuple(mesh.shape[a] for a in ("gx", "gy", "gz"))
    return jax.shard_map(
        functools.partial(shards, counts),
        mesh=mesh,
        in_specs=placed,
        out_specs=(P(None, None, "gx", None, "gz"), P(None, None, "gx", "gy", "gz")),
        check_vma=False,
    )
```

```python
import functools

import jax
import jax.numpy as jnp
from jax import lax
from jax.experimental import pallas as pl
from jax.experimental.pallas import tpu as pltpu
from jax.sharding import PartitionSpec as P

epsilon_value = 1e-05
step_size = 0.5
RAD = 4
MESH = pl.DeviceIdType.MESH
HIGH = lax.Precision.HIGHEST


def beta(offset):
    magnitude = jnp.abs(offset)
    interior = 2.0 / 3.0 - magnitude * magnitude + 0.5 * magnitude * magnitude * magnitude
    outside = jnp.maximum(2.0 - magnitude, 0.0)
    outside = outside * outside * outside / 6.0
    return jnp.where(magnitude < 1.0, interior, outside)


def beta_static(t):
    m = abs(t)
    if m < 1.0:
        return 2.0 / 3.0 - m * m + 0.5 * m * m * m
    return max(2.0 - m, 0.0) ** 3 / 6.0


def iota(shape, dim):
    return lax.broadcasted_iota(jnp.int32, shape, dim)


def lane_groups(lanes, groups, size):
    group = jnp.zeros_like(lanes)
    for n in range(1, groups + 1):
        group = group + (lanes >= n * size).astype(jnp.int32)
    return group, lanes - group * size


def split2(x):
    high = x.astype(jnp.bfloat16)
    low = (x - high.astype(jnp.float32)).astype(jnp.bfloat16)
    return high, low


def split3(x):
    high = x.astype(jnp.bfloat16)
    rest = x - high.astype(jnp.float32)
    mid = rest.astype(jnp.bfloat16)
    low = (rest - mid.astype(jnp.float32)).astype(jnp.bfloat16)
    return high, mid, low


def dot32(a, b):
    return jnp.dot(a, b, preferred_element_type=jnp.float32)


def dot_ones(x, ones_twice):
    high, mid, low = split3(x)
    depth = x.shape[1]
    return dot32(jnp.concatenate([high, mid], axis=1), ones_twice) + dot32(low, ones_twice[:depth])


def dot_split(x, table):
    high, low = split2(x)
    t_high, t_low = split2(table)
    return dot32(
        jnp.concatenate([high, low], axis=1), jnp.concatenate([t_high, t_high], axis=0)
    ) + dot32(high, t_low)


def force_kernel(
    counts, dims, img_hbm, vel_hbm, w_ref, own_ref,
    vol, vel, hz, pack, xs, t3, h5, acc, velp, ptile, joined, zrecv, slots, canvas,
    load, halo_send, halo_recv, z_send, z_recv, p_send, p_recv,
):
    nx, ny, nz = counts
    gx, gy, gz = lax.axis_index("gx"), lax.axis_index("gy"), lax.axis_index("gz")
    cx, cy, cz = dims
    bx, by, bz = cx // 8, cy // 8, cz // 8
    ly = vel.shape[3]
    wx, wz = bx + 4, bz + 4
    rows = cy + 16
    f32 = jnp.float32

    def exists(index, count, d):
        if d == 0:
            return True
        return index + d < count if d > 0 else index + d >= 0

    def valid(o):
        ok = None
        for index, count, d in zip((gx, gy, gz), counts, o):
            if d != 0:
                here = exists(index, count, d)
                ok = here if ok is None else ok & here
        return ok

    span = (-1, 0, 1)
    offsets = [(a, b, c) for c in span for a in span for b in span if (a, b, c) != (0, 0, 0)]
    offsets.sort(key=lambda o: abs(o[2]))
    peers = plane_peers(counts, bx)

    img = vol.at[:, RAD : RAD + cx, 8 : 8 + cy, :]
    load_images = pltpu.make_async_copy(img_hbm, img, load.at[0])
    load_velocity = pltpu.make_async_copy(vel_hbm, vel, load.at[1])
    load_images.start()
    load_velocity.start()

    barrier = pltpu.get_barrier_semaphore()

    def greet(px, py, pz):
        pl.semaphore_signal(
            barrier, inc=1, device_id={"gx": px, "gy": py, "gz": pz}, device_id_type=MESH
        )

    plane = [o for o in offsets if o[2] == 0]
    if ny > 2:
        plane = []
        for d, r in peers:

            @pl.when(True if d == 0 else exists(gx, nx, d))
            def _(d=d, r=r):
                greet(gx + d, lax.rem(gy + r, ny), gz)

    for o in plane + [o for o in offsets if o[2] != 0]:

        @pl.when(valid(o))
        def _(o=o):
            greet(gx + o[0], gy + o[1], gz + o[2])

    load_images.wait()

    lane = iota((cy, cz), 1)
    cell = lane // RAD
    edge_low = jnp.zeros((cy, cz), f32)
    edge_high = jnp.zeros((cy, cz), f32)
    for g in range(2 * cx):
        v = vol[g // cx, RAD + g % cx, 8 : 8 + cy]
        low = pltpu.roll(v, RAD * g, 1) if g else v
        shift = (RAD * g + RAD) % cz
        high = pltpu.roll(v, shift, 1) if shift else v
        edge_low = jnp.where(cell == g, low, edge_low)
        edge_high = jnp.where(cell == g, high, edge_high)
    pack[0] = edge_low
    pack[1] = edge_high

    def sides(index, count):
        return jnp.int32(index > 0) + jnp.int32(index < count - 1)

    near = (1 + sides(gx, nx)) * (1 + sides(gy, ny))
    beside = near * sides(gz, nz)
    if ny > 2:
        near = 0
        for d in sorted({d for d, _ in peers}):
            near = near + (ny if d == 0 else ny * jnp.int32(exists(gx, nx, d)))
    pl.semaphore_wait(barrier, near - 1 + beside)

    def halo_copy(n, o):
        dx, dy, dz = o
        src_y = {-1: (0, RAD), 0: (0, cy), 1: (cy - RAD, RAD)}[dy]
        dst_y = {-1: pl.ds(cy + 8, RAD), 0: pl.ds(8, cy), 1: pl.ds(8 - RAD, RAD)}[dy]
        if dz == 0:
            src_x = {-1: pl.ds(RAD, RAD), 0: pl.ds(RAD, cx), 1: pl.ds(cx, RAD)}[dx]
            dst_x = {-1: pl.ds(cx + RAD, RAD), 0: pl.ds(RAD, cx), 1: pl.ds(0, RAD)}[dx]
            src = vol.at[:, src_x, pl.ds(8 + src_y[0], src_y[1]), :]
            dst = vol.at[:, dst_x, dst_y, :]
        else:
            src = pack.at[(dz + 1) // 2, pl.ds(*src_y), :]
            dst = hz.at[(1 - dz) // 2, 1 - dx, dst_y, :]
        return pltpu.make_async_remote_copy(
            src_ref=src,
            dst_ref=dst,
            send_sem=halo_send.at[n],
            recv_sem=halo_recv.at[n],
            device_id={"gx": gx + dx, "gy": gy + dy, "gz": gz + dz},
            device_id_type=MESH,
        )

    for n, o in enumerate(offsets):

        @pl.when(valid(o))
        def _(n=n, o=o):
            halo_copy(n, o).start()

    load_velocity.wait()
    velocity_lane = iota((bz, cz), 1)
    velocity_row = iota((bz, cz), 0)
    take = (iota((8, ly), 1) == by * gy + iota((8, ly), 0) - 2) & (iota((8, ly), 0) >= 2)
    take = (take & (iota((8, ly), 0) < 2 + by)).astype(f32)
    for i in range(bx):
        placed = jnp.zeros((ly, cz), f32)
        for c in range(6):
            spot = (velocity_lane == velocity_row + c * wz + 2).astype(f32)
            placed = placed + jnp.dot(
                vel[c // 3, c % 3, i], spot, precision=HIGH, preferred_element_type=f32
            )
        velp[i] = jnp.dot(take, placed, precision=HIGH, preferred_element_type=f32)
    acc[...] = jnp.zeros(acc.shape, f32)

    band = (jnp.abs(iota((cz, cz), 0) - iota((cz, cz), 1)) <= RAD).astype(f32)
    band = jnp.concatenate([band, band], axis=0).astype(jnp.bfloat16)

    def edge_matrix(side, part, image):
        row, col = iota((cz, cz), 0), iota((cz, cz), 1)
        row_x = (row // RAD) % cx + cx * (part - 1)
        dz = row % RAD
        col_x = col // (2 * RAD)
        place = col % (2 * RAD)
        near = (row // (RAD * cx) == image) & (jnp.abs(row_x - col_x) <= RAD)
        if side == 0:
            reach = (place >= RAD) & (place - RAD <= dz)
        else:
            reach = (place < RAD) & (place >= dz)
        return (near & reach).astype(f32)

    def edge_table(parts, image):
        whole = jnp.concatenate(
            [edge_matrix(s, p, image) for s in range(2) for p in parts], axis=0
        )
        return jnp.concatenate([whole, whole], axis=0).astype(jnp.bfloat16)

    middle = (1,)
    outer = (0, 2)
    tables = {parts: [edge_table(parts, n) for n in range(2)] for parts in (middle, outer)}

    def arrive(wanted):
        for n, o in enumerate(offsets):
            if (o[0] != 0) == wanted:

                @pl.when(valid(tuple(-d for d in o)))
                def _(n=n, o=o):
                    halo_copy(n, o).wait_recv()

    @pl.when(gx == 0)
    def _():
        vol[:, 0:RAD] = jnp.zeros((2, RAD, rows, cz), f32)
        hz[:, 0] = jnp.zeros((2, rows, cz), f32)

    @pl.when(gx == nx - 1)
    def _():
        vol[:, cx + RAD :] = jnp.zeros((2, RAD, rows, cz), f32)
        hz[:, 2] = jnp.zeros((2, rows, cz), f32)

    @pl.when(gy == 0)
    def _():
        vol[:, :, 0:8] = jnp.zeros((2, cx + 2 * RAD, 8, cz), f32)
        hz[:, :, 0:8] = jnp.zeros((2, 3, 8, cz), f32)

    @pl.when(gy == ny - 1)
    def _():
        vol[:, :, 8 + cy :] = jnp.zeros((2, cx + 2 * RAD, 8, cz), f32)
        hz[:, :, 8 + cy :] = jnp.zeros((2, 3, 8, cz), f32)

    @pl.when(gz == 0)
    def _():
        hz[0] = jnp.zeros((3, rows, cz), f32)

    @pl.when(gz == nz - 1)
    def _():
        hz[1] = jnp.zeros((3, rows, cz), f32)

    def window_rows(count):
        tall = cy + 8
        t3[0:count] = (
            xs[0:count, 4 : 4 + tall] + xs[0:count, 5 : 5 + tall] + xs[0:count, 6 : 6 + tall]
        )
        return t3[0:count, 0:cy] + t3[0:count, 3 : 3 + cy] + t3[0:count, 6 : 6 + cy]

    def edge_sums(parts):
        count = 2 * len(parts)
        for s in range(2):
            for m, p in enumerate(parts):
                t = hz[s, p]
                n = s * len(parts) + m
                xs[n] = t
                xs[count + n] = t * t
                xs[2 * count + n] = t * pltpu.roll(t, cz // 2, 1)
        sums = window_rows(3 * count)
        kinds = jnp.concatenate(
            [
                jnp.concatenate([sums[kind * count + n] for n in range(count)], axis=1)
                for kind in range(3)
            ],
            axis=0,
        )
        fixed_edge = dot_ones(kinds, tables[parts][0])
        moving_edge = dot_ones(kinds[0 : 2 * cy], tables[parts][1])
        return [
            fixed_edge[0:cy],
            moving_edge[0:cy],
            fixed_edge[cy : 2 * cy],
            moving_edge[cy : 2 * cy],
            fixed_edge[2 * cy :],
        ]

    arrive(False)
    for k, value in enumerate(edge_sums(middle)):
        h5[k] = value
    h5[5] = jnp.where(
        lane % RAD == RAD - 1, hz[0, 1, 8 : 8 + cy], pltpu.roll(hz[1, 1, 8 : 8 + cy], 2, 1)
    )

    step = 4
    steps = cx // step

    def group(g, carry):
        first = g * step
        fs = [vol[0, first + d] for d in range(step + 8)]
        ms = [vol[1, first + d] for d in range(step + 8)]
        for k in range(5):
            if k == 0:
                a = fs
            elif k == 1:
                a = ms
            elif k == 2:
                a = [f * f for f in fs]
            elif k == 3:
                a = [m * m for m in ms]
            else:
                a = [f * m for f, m in zip(fs, ms)]
            common = a[3] + a[4] + a[5] + (a[6] + a[7] + a[8])
            left2 = a[1] + a[2]
            right2 = a[9] + a[10]
            xs[k * step] = common + (left2 + a[0])
            xs[k * step + 1] = common + (left2 + a[9])
            xs[k * step + 2] = common + (right2 + a[2])
            xs[k * step + 3] = common + (right2 + a[11])
        flat = window_rows(5 * step).reshape(5 * step * cy, cz)
        sums = dot_ones(flat, band).reshape(5, step, cy, cz)
        inner = (lane < RAD) | (lane >= cz - RAD)
        pulls = []
        for s in range(step):
            x = first + s
            shift = lax.rem(2 * cz - RAD - 2 * RAD * x, cz)
            mean = []
            for k in range(5):
                extra = jnp.where(inner, pltpu.roll(h5[k], shift, 1), 0.0)
                mean.append((sums[k, s] + extra) * (1.0 / 729.0))
            m_f, m_m, q_f, q_m, q_fm = mean
            var_f = q_f - m_f * m_f + epsilon_value
            var_m = q_m - m_m * m_m + epsilon_value
            cov = q_fm - m_f * m_m
            slope_f = cov / var_f
            slope_m = cov / var_m
            factor = (2.0 * 0.5 * step_size) * slope_f / var_m
            own_f = vol[0, x + RAD, 8 : 8 + cy]
            own_m = vol[1, x + RAD, 8 : 8 + cy]
            cen_f = own_f - m_f
            cen_m = own_m - m_m
            pull = [factor * (cen_m - slope_f * cen_f), factor * (cen_f - slope_m * cen_m)]
            forces = []
            for h, own in ((0, own_f), (1, own_m)):
                along_x = (
                    vol[h, x + RAD + 1, 8 : 8 + cy] - vol[h, x + RAD - 1, 8 : 8 + cy]
                )
                along_y = vol[h, x + RAD, 9 : 9 + cy] - vol[h, x + RAD, 7 : 7 + cy]
                turn = lax.rem(2 * cz - 3 - RAD * (h * cx + x), cz)
                beyond = pltpu.roll(h5[5], turn, 1)
                above = jnp.where(lane == cz - 1, beyond, pltpu.roll(own, cz - 1, 1))
                below = jnp.where(lane == 0, beyond, pltpu.roll(own, 1, 1))
                forces += [pull[h] * along_x, pull[h] * along_y, pull[h] * (above - below)]
            pulls.append(forces)
        half = lax.rem(g, 2)
        base = g // 2 + half
        for t in range(4):
            weights = []
            for s in range(step):
                low = beta_static(2 - t + (s - 3.5) / 8.0)
                high = beta_static(1 - t + (s + 4 - 3.5) / 8.0)
                weights.append(jnp.where(half == 0, f32(low), f32(high)))
            for c in range(6):
                total = pulls[0][c] * weights[0]
                for s in range(1, step):
                    total = total + pulls[s][c] * weights[s]
                acc[c, base + t] = acc[c, base + t] + total
        return carry

    lax.fori_loop(1, steps - 1, group, 0)
    arrive(True)
    for k, value in enumerate(edge_sums(outer)):
        h5[k] = h5[k] + value
    lax.fori_loop(0, 2, lambda n, carry: group(n * (steps - 1), carry), 0)

    points_lane = iota((cz, cz), 1)
    _, table_k = lane_groups(points_lane, 6, wz)
    position = iota((cz, cz), 0) - 8 * (table_k - 2)
    table_z = beta((position.astype(f32) - 3.5) / 8.0)
    along = dot_split(acc[...].reshape(6 * wx * cy, cz), table_z).reshape(6, wx, cy, cz)
    lane_c, _ = lane_groups(lane, 6, wz)
    row_j = iota((8, cy), 0)
    table_y = beta((iota((8, cy), 1) - 8 * (row_j - 2)).astype(f32) / 8.0 - 3.5 / 8.0)
    table_y = table_y[: by + 4]
    for i in range(wx):
        packed = jnp.zeros((cy, cz), f32)
        for c in range(6):
            packed = jnp.where(lane_c == c, along[c, i], packed)
        ptile[i] = jnp.dot(
            table_y, packed, precision=HIGH, preferred_element_type=f32
        )
        if 2 <= i < 2 + bx:
            ptile[i] = ptile[i] + velp[i - 2]

    def z_copy(n):
        d = 1 - 2 * n
        return pltpu.make_async_remote_copy(
            src_ref=ptile,
            dst_ref=zrecv.at[n],
            send_sem=z_send.at[n],
            recv_sem=z_recv.at[n],
            device_id={"gx": gx, "gy": gy, "gz": gz + d},
            device_id_type=MESH,
        )

    for n in range(2):

        @pl.when(exists(gz, nz, 1 - 2 * n))
        def _(n=n):
            z_copy(n).start()

    for n in range(2):
        here = exists(gz, nz, 2 * n - 1)

        @pl.when(here)
        def _(n=n):
            z_copy(n).wait_recv()

        @pl.when(jnp.logical_not(here))
        def _(n=n):
            zrecv[n] = jnp.zeros(ptile.shape, f32)

    tile_rows = wx * (by + 4)
    tile_lane = iota((tile_rows, cz), 1)
    _, tile_k = lane_groups(tile_lane, 6, wz)
    from_left = pltpu.roll(zrecv[0].reshape(tile_rows, cz), cz - bz, 1)
    from_right = pltpu.roll(zrecv[1].reshape(tile_rows, cz), bz, 1)
    total = (
        ptile[...].reshape(tile_rows, cz)
        + jnp.where(tile_k < 4, from_left, 0.0)
        + jnp.where(tile_k >= bz, from_right, 0.0)
    )
    joined[...] = total.reshape(ptile.shape)
    far = max(d for d, _ in peers)

    def shared(d):
        here = max(0, bx * d)
        there = max(0, -bx * d)
        return here, there, wx - bx * abs(d)

    def p_copy(n, d, r):
        here, there, size = shared(d)
        return pltpu.make_async_remote_copy(
            src_ref=joined.at[pl.ds(here, size)],
            dst_ref=slots.at[far + d, gy, pl.ds(there, size)],
            send_sem=p_send.at[n],
            recv_sem=p_recv.at[n],
            device_id={"gx": gx + d, "gy": lax.rem(gy + r, ny), "gz": gz},
            device_id_type=MESH,
        )

    for n, (d, r) in enumerate(peers):

        @pl.when(True if d == 0 else exists(gx, nx, d))
        def _(n=n, d=d, r=r):
            p_copy(n, d, r).start()

    slots[far, gy] = joined[...]
    canvas[...] = jnp.zeros(canvas.shape, f32)
    for d in sorted({d for d, _ in peers}, key=abs):

        @pl.when(True if d == 0 else exists(gx, nx, -d))
        def _(d=d):
            for n, (e, r) in enumerate(peers):
                if e == d:
                    p_copy(n, d, r).wait_recv()
            _, there, size = shared(d)
            for b in range(ny):
                spot = (slice(there, there + size), slice(by * b, by * b + by + 4))
                canvas[spot] = canvas[spot] + slots[far + d, b, there : there + size]

    tall = canvas.shape[1]
    shape = (wx, tall, cz)
    point_c, point_k = lane_groups(iota(shape, 2), 6, wz)
    global_i = bx * gx - 2 + iota(shape, 0)
    global_k = bz * gz - 2 + point_k
    row = iota(shape, 1)
    inside = (point_c < 6) & (global_i >= 0) & (global_i < bx * nx)
    inside = inside & (global_k >= 0) & (global_k < bz * nz)
    inside = inside & (row >= 2) & (row < 2 + ly)
    canvas[...] = jnp.where(inside, canvas[...], 0.0)
    own_ref[...] = canvas[2 : 2 + bx]
    window = canvas[:, 0 : by + 4]
    for b in range(1, ny):
        window = jnp.where(gy == b, canvas[:, by * b : by * b + by + 4], window)
    w_ref[...] = window

    for n, o in enumerate(offsets):

        @pl.when(valid(o))
        def _(n=n, o=o):
            halo_copy(n, o).wait_send()

    for n in range(2):

        @pl.when(exists(gz, nz, 1 - 2 * n))
        def _(n=n):
            z_copy(n).wait_send()

    for n, (d, r) in enumerate(peers):

        @pl.when(True if d == 0 else exists(gx, nx, d))
        def _(n=n, d=d, r=r):
            p_copy(n, d, r).wait_send()


def plane_peers(counts, bx):
    nx, ny, _ = counts
    far = min(nx - 1, (bx + 3) // bx)
    pairs = [(d, r) for d in range(-far, far + 1) for r in range(ny)]
    return [pair for pair in pairs if pair != (0, 0)]


def field_kernel(w_ref, own_ref, nv_ref, out_hbm, spread, held, done):
    cx, cy, cz = held.shape[1:]
    ly = nv_ref.shape[3]
    bx, by, bz = cx // 8, cy // 8, cz // 8
    wx, wz = bx + 4, bz + 4
    wy = by + 4
    f32 = jnp.float32
    row = iota((cz, cz), 0)
    group, place = lane_groups(row, 6, wz)
    table = beta(((iota((cz, cz), 1) - 8 * (place - 2)).astype(f32) - 3.5) / 8.0)
    flat = w_ref[...].reshape(wx * wy, cz)
    lane_c, _ = lane_groups(iota((wx * wy, cz), 1), 6, wz)
    stack = jnp.concatenate([jnp.where(lane_c == c, flat, 0.0) for c in range(6)], axis=0)
    spread[...] = dot_split(stack, table).reshape(6, wx, wy, cz)
    sub = (iota((8, cz), 0).astype(f32) - 3.5) / 8.0
    taps = [beta(2.0 - t + sub) for t in range(5)]
    for c in range(6):
        for b in range(by):
            lines = []
            for i in range(wx):
                total = None
                for t in range(5):
                    term = taps[t] * spread[c, i, b + t : b + t + 1]
                    total = term if total is None else total + term
                lines.append(total)
            for x in range(cx):
                block, s = x // 8, x % 8
                half = s // 4
                total = None
                for t in range(half, half + 4):
                    term = beta_static(2 - t + (s - 3.5) / 8.0) * lines[block + t]
                    total = term if total is None else total + term
                held[c, x, 8 * b : 8 * b + 8] = total.astype(jnp.bfloat16)
        pltpu.make_async_copy(held.at[c], out_hbm.at[c // 3, c % 3], done.at[c]).start()
    for i in range(bx):
        for c in range(6):
            moved = own_ref[i]
            moved = pltpu.roll(moved, cz - (c * wz + 2), 1)
            nv_ref[c // 3, c % 3, i] = moved[2 : 2 + ly, 0:bz]
    for c in range(6):
        pltpu.make_async_copy(held.at[c], out_hbm.at[c // 3, c % 3], done.at[c]).wait()


def shards(counts, images, velocity):
    nx, ny, nz = counts
    _, cx, cy, cz = images.shape
    bx, by, bz = cx // 8, cy // 8, cz // 8
    wy = by + 4
    tall = -(-(by * ny + 4) // 8) * 8
    rows = cy + 16
    f32 = jnp.float32
    vmem = pl.BlockSpec(memory_space=pltpu.VMEM)
    hbm = pl.BlockSpec(memory_space=pl.ANY)
    offsets = 26
    peers = plane_peers(counts, bx)
    far = max(d for d, _ in peers)
    wx = bx + 4
    window, own = pl.pallas_call(
        functools.partial(force_kernel, counts, (cx, cy, cz)),
        out_shape=(
            jax.ShapeDtypeStruct((wx, wy, cz), f32),
            jax.ShapeDtypeStruct((bx, tall, cz), f32),
        ),
        in_specs=[hbm, hbm],
        out_specs=(vmem, vmem),
        scratch_shapes=[
            pltpu.VMEM((2, cx + 2 * RAD, rows, cz), f32),
            pltpu.VMEM(velocity.shape, f32),
            pltpu.VMEM((2, 3, rows, cz), f32),
            pltpu.VMEM((2, cy, cz), f32),
            pltpu.VMEM((20, rows, cz), f32),
            pltpu.VMEM((20, cy + 8, cz), f32),
            pltpu.VMEM((6, cy, cz), f32),
            pltpu.VMEM((6, wx, cy, cz), f32),
            pltpu.VMEM((bx, wy, cz), f32),
            pltpu.VMEM((wx, wy, cz), f32),
            pltpu.VMEM((wx, wy, cz), f32),
            pltpu.VMEM((2, wx, wy, cz), f32),
            pltpu.VMEM((2 * far + 1, ny, wx, wy, cz), f32),
            pltpu.VMEM((wx, tall, cz), f32),
            pltpu.SemaphoreType.DMA((2,)),
            pltpu.SemaphoreType.DMA((offsets,)),
            pltpu.SemaphoreType.DMA((offsets,)),
            pltpu.SemaphoreType.DMA((2,)),
            pltpu.SemaphoreType.DMA((2,)),
            pltpu.SemaphoreType.DMA((len(peers),)),
            pltpu.SemaphoreType.DMA((len(peers),)),
        ],
        compiler_params=pltpu.CompilerParams(collective_id=0, has_side_effects=True),
        name="forces",
    )(images, velocity)
    new_velocity, field = pl.pallas_call(
        field_kernel,
        out_shape=(
            jax.ShapeDtypeStruct(velocity.shape, f32),
            jax.ShapeDtypeStruct((2, 3, cx, cy, cz), jnp.bfloat16),
        ),
        in_specs=[vmem, vmem],
        out_specs=(vmem, hbm),
        scratch_shapes=[
            pltpu.VMEM((6, wx, wy, cz), f32),
            pltpu.VMEM((6, cx, cy, cz), jnp.bfloat16),
            pltpu.SemaphoreType.DMA((6,)),
        ],
        name="field",
    )(window, own)
    return new_velocity, field


def solution(mesh):
    placed = (P(None, "gx", "gy", "gz"), P(None, None, "gx", None, "gz"))
    counts = tuple(mesh.shape[a] for a in ("gx", "gy", "gz"))
    return jax.shard_map(
        functools.partial(shards, counts),
        mesh=mesh,
        in_specs=placed,
        out_specs=(P(None, None, "gx", None, "gz"), P(None, None, "gx", "gy", "gz")),
        check_vma=False,
    )
```

```python
import functools

import jax
import jax.numpy as jnp
from jax import lax
from jax.experimental import pallas as pl
from jax.experimental.pallas import tpu as pltpu
from jax.sharding import PartitionSpec as P

epsilon_value = 1e-05
step_size = 0.5
RAD = 4
MESH = pl.DeviceIdType.MESH
HIGH = lax.Precision.HIGHEST


def beta(offset):
    magnitude = jnp.abs(offset)
    interior = 2.0 / 3.0 - magnitude * magnitude + 0.5 * magnitude * magnitude * magnitude
    outside = jnp.maximum(2.0 - magnitude, 0.0)
    outside = outside * outside * outside / 6.0
    return jnp.where(magnitude < 1.0, interior, outside)


def beta_static(t):
    m = abs(t)
    if m < 1.0:
        return 2.0 / 3.0 - m * m + 0.5 * m * m * m
    return max(2.0 - m, 0.0) ** 3 / 6.0


def iota(shape, dim):
    return lax.broadcasted_iota(jnp.int32, shape, dim)


def lane_groups(lanes, groups, size):
    group = jnp.zeros_like(lanes)
    for n in range(1, groups + 1):
        group = group + (lanes >= n * size).astype(jnp.int32)
    return group, lanes - group * size


def split2(x):
    high = x.astype(jnp.bfloat16)
    low = (x - high.astype(jnp.float32)).astype(jnp.bfloat16)
    return high, low


def split3(x):
    high = x.astype(jnp.bfloat16)
    rest = x - high.astype(jnp.float32)
    mid = rest.astype(jnp.bfloat16)
    low = (rest - mid.astype(jnp.float32)).astype(jnp.bfloat16)
    return high, mid, low


def dot32(a, b):
    return jnp.dot(a, b, preferred_element_type=jnp.float32)


def dot_ones(x, ones_twice):
    high, mid, low = split3(x)
    depth = x.shape[1]
    return dot32(jnp.concatenate([high, mid], axis=1), ones_twice) + dot32(low, ones_twice[:depth])


def dot_split(x, table):
    high, low = split2(x)
    t_high, t_low = split2(table)
    return dot32(
        jnp.concatenate([high, low], axis=1), jnp.concatenate([t_high, t_high], axis=0)
    ) + dot32(high, t_low)


def force_kernel(
    counts, dims, img_hbm, vel_hbm, w_ref, own_ref,
    vol, vel, hz, pack, xs, t3, h5, acc, velp, ptile, joined, zrecv, slots, canvas,
    load, halo_send, halo_recv, z_send, z_recv, p_send, p_recv,
):
    nx, ny, nz = counts
    gx, gy, gz = lax.axis_index("gx"), lax.axis_index("gy"), lax.axis_index("gz")
    cx, cy, cz = dims
    bx, by, bz = cx // 8, cy // 8, cz // 8
    ly = vel.shape[3]
    wx, wz = bx + 4, bz + 4
    rows = cy + 16
    f32 = jnp.float32

    def exists(index, count, d):
        if d == 0:
            return True
        return index + d < count if d > 0 else index + d >= 0

    def valid(o):
        ok = None
        for index, count, d in zip((gx, gy, gz), counts, o):
            if d != 0:
                here = exists(index, count, d)
                ok = here if ok is None else ok & here
        return ok

    span = (-1, 0, 1)
    offsets = [(a, b, c) for c in span for a in span for b in span if (a, b, c) != (0, 0, 0)]
    offsets.sort(key=lambda o: abs(o[2]))
    peers = plane_peers(counts, bx)

    img = vol.at[:, RAD : RAD + cx, 8 : 8 + cy, :]
    load_images = pltpu.make_async_copy(img_hbm, img, load.at[0])
    load_velocity = pltpu.make_async_copy(vel_hbm, vel, load.at[1])
    load_images.start()
    load_velocity.start()

    barrier = pltpu.get_barrier_semaphore()

    def greet(px, py, pz):
        pl.semaphore_signal(
            barrier, inc=1, device_id={"gx": px, "gy": py, "gz": pz}, device_id_type=MESH
        )

    plane = [o for o in offsets if o[2] == 0]
    if ny > 2:
        plane = []
        for d, r in peers:

            @pl.when(True if d == 0 else exists(gx, nx, d))
            def _(d=d, r=r):
                greet(gx + d, lax.rem(gy + r, ny), gz)

    for o in plane + [o for o in offsets if o[2] != 0]:

        @pl.when(valid(o))
        def _(o=o):
            greet(gx + o[0], gy + o[1], gz + o[2])

    load_images.wait()

    lane = iota((cy, cz), 1)
    cell = lane // RAD
    edge_low = jnp.zeros((cy, cz), f32)
    edge_high = jnp.zeros((cy, cz), f32)
    for g in range(2 * cx):
        v = vol[g // cx, RAD + g % cx, 8 : 8 + cy]
        low = pltpu.roll(v, RAD * g, 1) if g else v
        shift = (RAD * g + RAD) % cz
        high = pltpu.roll(v, shift, 1) if shift else v
        edge_low = jnp.where(cell == g, low, edge_low)
        edge_high = jnp.where(cell == g, high, edge_high)
    pack[0] = edge_low
    pack[1] = edge_high

    def sides(index, count):
        return jnp.int32(index > 0) + jnp.int32(index < count - 1)

    near = (1 + sides(gx, nx)) * (1 + sides(gy, ny))
    beside = near * sides(gz, nz)
    if ny > 2:
        near = 0
        for d in sorted({d for d, _ in peers}):
            near = near + (ny if d == 0 else ny * jnp.int32(exists(gx, nx, d)))
    pl.semaphore_wait(barrier, near - 1 + beside)

    def halo_copy(n, o):
        dx, dy, dz = o
        src_y = {-1: (0, RAD), 0: (0, cy), 1: (cy - RAD, RAD)}[dy]
        dst_y = {-1: pl.ds(cy + 8, RAD), 0: pl.ds(8, cy), 1: pl.ds(8 - RAD, RAD)}[dy]
        if dz == 0:
            src_x = {-1: pl.ds(RAD, RAD), 0: pl.ds(RAD, cx), 1: pl.ds(cx, RAD)}[dx]
            dst_x = {-1: pl.ds(cx + RAD, RAD), 0: pl.ds(RAD, cx), 1: pl.ds(0, RAD)}[dx]
            src = vol.at[:, src_x, pl.ds(8 + src_y[0], src_y[1]), :]
            dst = vol.at[:, dst_x, dst_y, :]
        else:
            src = pack.at[(dz + 1) // 2, pl.ds(*src_y), :]
            dst = hz.at[(1 - dz) // 2, 1 - dx, dst_y, :]
        return pltpu.make_async_remote_copy(
            src_ref=src,
            dst_ref=dst,
            send_sem=halo_send.at[n],
            recv_sem=halo_recv.at[n],
            device_id={"gx": gx + dx, "gy": gy + dy, "gz": gz + dz},
            device_id_type=MESH,
        )

    for n, o in enumerate(offsets):

        @pl.when(valid(o))
        def _(n=n, o=o):
            halo_copy(n, o).start()

    load_velocity.wait()
    velocity_lane = iota((bz, cz), 1)
    velocity_row = iota((bz, cz), 0)
    take = (iota((8, ly), 1) == by * gy + iota((8, ly), 0) - 2) & (iota((8, ly), 0) >= 2)
    take = (take & (iota((8, ly), 0) < 2 + by)).astype(f32)
    for i in range(bx):
        placed = jnp.zeros((ly, cz), f32)
        for c in range(6):
            spot = (velocity_lane == velocity_row + c * wz + 2).astype(f32)
            placed = placed + jnp.dot(
                vel[c // 3, c % 3, i], spot, precision=HIGH, preferred_element_type=f32
            )
        velp[i] = jnp.dot(take, placed, precision=HIGH, preferred_element_type=f32)
    acc[...] = jnp.zeros(acc.shape, f32)

    band = (jnp.abs(iota((cz, cz), 0) - iota((cz, cz), 1)) <= RAD).astype(f32)
    band = jnp.concatenate([band, band], axis=0).astype(jnp.bfloat16)

    def edge_matrix(side, part, image):
        row, col = iota((cz, cz), 0), iota((cz, cz), 1)
        row_x = (row // RAD) % cx + cx * (part - 1)
        dz = row % RAD
        col_x = col // (2 * RAD)
        place = col % (2 * RAD)
        near = (row // (RAD * cx) == image) & (jnp.abs(row_x - col_x) <= RAD)
        if side == 0:
            reach = (place >= RAD) & (place - RAD <= dz)
        else:
            reach = (place < RAD) & (place >= dz)
        return (near & reach).astype(f32)

    def edge_table(parts, image):
        whole = jnp.concatenate(
            [edge_matrix(s, p, image) for s in range(2) for p in parts], axis=0
        )
        return jnp.concatenate([whole, whole], axis=0).astype(jnp.bfloat16)

    middle = (1,)
    outer = (0, 2)
    tables = {parts: [edge_table(parts, n) for n in range(2)] for parts in (middle, outer)}

    def arrive(wanted):
        for n, o in enumerate(offsets):
            if (o[0] != 0) == wanted:

                @pl.when(valid(tuple(-d for d in o)))
                def _(n=n, o=o):
                    halo_copy(n, o).wait_recv()

    @pl.when(gx == 0)
    def _():
        vol[:, 0:RAD] = jnp.zeros((2, RAD, rows, cz), f32)
        hz[:, 0] = jnp.zeros((2, rows, cz), f32)

    @pl.when(gx == nx - 1)
    def _():
        vol[:, cx + RAD :] = jnp.zeros((2, RAD, rows, cz), f32)
        hz[:, 2] = jnp.zeros((2, rows, cz), f32)

    @pl.when(gy == 0)
    def _():
        vol[:, :, 0:8] = jnp.zeros((2, cx + 2 * RAD, 8, cz), f32)
        hz[:, :, 0:8] = jnp.zeros((2, 3, 8, cz), f32)

    @pl.when(gy == ny - 1)
    def _():
        vol[:, :, 8 + cy :] = jnp.zeros((2, cx + 2 * RAD, 8, cz), f32)
        hz[:, :, 8 + cy :] = jnp.zeros((2, 3, 8, cz), f32)

    @pl.when(gz == 0)
    def _():
        hz[0] = jnp.zeros((3, rows, cz), f32)

    @pl.when(gz == nz - 1)
    def _():
        hz[1] = jnp.zeros((3, rows, cz), f32)

    def window_rows(count):
        tall = cy + 8
        t3[0:count] = (
            xs[0:count, 4 : 4 + tall] + xs[0:count, 5 : 5 + tall] + xs[0:count, 6 : 6 + tall]
        )
        return t3[0:count, 0:cy] + t3[0:count, 3 : 3 + cy] + t3[0:count, 6 : 6 + cy]

    def edge_sums(parts):
        count = 2 * len(parts)
        for s in range(2):
            for m, p in enumerate(parts):
                t = hz[s, p]
                n = s * len(parts) + m
                xs[n] = t
                xs[count + n] = t * t
                xs[2 * count + n] = t * pltpu.roll(t, cz // 2, 1)
        sums = window_rows(3 * count)
        kinds = jnp.concatenate(
            [
                jnp.concatenate([sums[kind * count + n] for n in range(count)], axis=1)
                for kind in range(3)
            ],
            axis=0,
        )
        fixed_edge = dot_ones(kinds, tables[parts][0])
        moving_edge = dot_ones(kinds[0 : 2 * cy], tables[parts][1])
        return [
            fixed_edge[0:cy],
            moving_edge[0:cy],
            fixed_edge[cy : 2 * cy],
            moving_edge[cy : 2 * cy],
            fixed_edge[2 * cy :],
        ]

    arrive(False)
    for k, value in enumerate(edge_sums(middle)):
        h5[k] = value
    h5[5] = jnp.where(
        lane % RAD == RAD - 1, hz[0, 1, 8 : 8 + cy], pltpu.roll(hz[1, 1, 8 : 8 + cy], 2, 1)
    )

    step = 4
    steps = cx // step

    def group(g, carry):
        first = g * step
        fs = [vol[0, first + d] for d in range(step + 8)]
        ms = [vol[1, first + d] for d in range(step + 8)]
        for k in range(5):
            if k == 0:
                a = fs
            elif k == 1:
                a = ms
            elif k == 2:
                a = [f * f for f in fs]
            elif k == 3:
                a = [m * m for m in ms]
            else:
                a = [f * m for f, m in zip(fs, ms)]
            common = a[3] + a[4] + a[5] + (a[6] + a[7] + a[8])
            left2 = a[1] + a[2]
            right2 = a[9] + a[10]
            xs[k * step] = common + (left2 + a[0])
            xs[k * step + 1] = common + (left2 + a[9])
            xs[k * step + 2] = common + (right2 + a[2])
            xs[k * step + 3] = common + (right2 + a[11])
        flat = window_rows(5 * step).reshape(5 * step * cy, cz)
        sums = dot_ones(flat, band).reshape(5, step, cy, cz)
        inner = (lane < RAD) | (lane >= cz - RAD)
        pulls = []
        for s in range(step):
            x = first + s
            shift = lax.rem(2 * cz - RAD - 2 * RAD * x, cz)
            mean = []
            for k in range(5):
                extra = jnp.where(inner, pltpu.roll(h5[k], shift, 1), 0.0)
                mean.append((sums[k, s] + extra) * (1.0 / 729.0))
            m_f, m_m, q_f, q_m, q_fm = mean
            var_f = q_f - m_f * m_f + epsilon_value
            var_m = q_m - m_m * m_m + epsilon_value
            cov = q_fm - m_f * m_m
            slope_f = cov / var_f
            slope_m = cov / var_m
            factor = (2.0 * 0.5 * step_size) * slope_f / var_m
            own_f = vol[0, x + RAD, 8 : 8 + cy]
            own_m = vol[1, x + RAD, 8 : 8 + cy]
            cen_f = own_f - m_f
            cen_m = own_m - m_m
            pull = [factor * (cen_m - slope_f * cen_f), factor * (cen_f - slope_m * cen_m)]
            forces = []
            for h, own in ((0, own_f), (1, own_m)):
                along_x = (
                    vol[h, x + RAD + 1, 8 : 8 + cy] - vol[h, x + RAD - 1, 8 : 8 + cy]
                )
                along_y = vol[h, x + RAD, 9 : 9 + cy] - vol[h, x + RAD, 7 : 7 + cy]
                turn = lax.rem(2 * cz - 3 - RAD * (h * cx + x), cz)
                beyond = pltpu.roll(h5[5], turn, 1)
                above = jnp.where(lane == cz - 1, beyond, pltpu.roll(own, cz - 1, 1))
                below = jnp.where(lane == 0, beyond, pltpu.roll(own, 1, 1))
                forces += [pull[h] * along_x, pull[h] * along_y, pull[h] * (above - below)]
            pulls.append(forces)
        half = lax.rem(g, 2)
        base = g // 2 + half
        for t in range(4):
            weights = []
            for s in range(step):
                low = beta_static(2 - t + (s - 3.5) / 8.0)
                high = beta_static(1 - t + (s + 4 - 3.5) / 8.0)
                weights.append(jnp.where(half == 0, f32(low), f32(high)))
            for c in range(6):
                total = pulls[0][c] * weights[0]
                for s in range(1, step):
                    total = total + pulls[s][c] * weights[s]
                acc[c, base + t] = acc[c, base + t] + total
        return carry

    lax.fori_loop(1, steps - 1, group, 0)
    arrive(True)
    for k, value in enumerate(edge_sums(outer)):
        h5[k] = h5[k] + value
    lax.fori_loop(0, 2, lambda n, carry: group(n * (steps - 1), carry), 0)

    points_lane = iota((cz, cz), 1)
    _, table_k = lane_groups(points_lane, 6, wz)
    position = iota((cz, cz), 0) - 8 * (table_k - 2)
    table_z = beta((position.astype(f32) - 3.5) / 8.0)
    along = dot_split(acc[...].reshape(6 * wx * cy, cz), table_z).reshape(6, wx, cy, cz)
    lane_c, _ = lane_groups(lane, 6, wz)
    row_j = iota((8, cy), 0)
    table_y = beta((iota((8, cy), 1) - 8 * (row_j - 2)).astype(f32) / 8.0 - 3.5 / 8.0)
    table_y = table_y[: by + 4]
    for i in range(wx):
        packed = jnp.zeros((cy, cz), f32)
        for c in range(6):
            packed = jnp.where(lane_c == c, along[c, i], packed)
        ptile[i] = jnp.dot(
            table_y, packed, precision=HIGH, preferred_element_type=f32
        )
        if 2 <= i < 2 + bx:
            ptile[i] = ptile[i] + velp[i - 2]

    def z_copy(n):
        d = 1 - 2 * n
        return pltpu.make_async_remote_copy(
            src_ref=ptile,
            dst_ref=zrecv.at[n],
            send_sem=z_send.at[n],
            recv_sem=z_recv.at[n],
            device_id={"gx": gx, "gy": gy, "gz": gz + d},
            device_id_type=MESH,
        )

    for n in range(2):

        @pl.when(exists(gz, nz, 1 - 2 * n))
        def _(n=n):
            z_copy(n).start()

    for n in range(2):
        here = exists(gz, nz, 2 * n - 1)

        @pl.when(here)
        def _(n=n):
            z_copy(n).wait_recv()

        @pl.when(jnp.logical_not(here))
        def _(n=n):
            zrecv[n] = jnp.zeros(ptile.shape, f32)

    tile_rows = wx * (by + 4)
    tile_lane = iota((tile_rows, cz), 1)
    _, tile_k = lane_groups(tile_lane, 6, wz)
    from_left = pltpu.roll(zrecv[0].reshape(tile_rows, cz), cz - bz, 1)
    from_right = pltpu.roll(zrecv[1].reshape(tile_rows, cz), bz, 1)
    total = (
        ptile[...].reshape(tile_rows, cz)
        + jnp.where(tile_k < 4, from_left, 0.0)
        + jnp.where(tile_k >= bz, from_right, 0.0)
    )
    joined[...] = total.reshape(ptile.shape)
    far = max(d for d, _ in peers)

    def shared(d):
        here = max(0, bx * d)
        there = max(0, -bx * d)
        return here, there, wx - bx * abs(d)

    def p_copy(n, d, r):
        here, there, size = shared(d)
        return pltpu.make_async_remote_copy(
            src_ref=joined.at[pl.ds(here, size)],
            dst_ref=slots.at[far + d, gy, pl.ds(there, size)],
            send_sem=p_send.at[n],
            recv_sem=p_recv.at[n],
            device_id={"gx": gx + d, "gy": lax.rem(gy + r, ny), "gz": gz},
            device_id_type=MESH,
        )

    for n, (d, r) in enumerate(peers):

        @pl.when(True if d == 0 else exists(gx, nx, d))
        def _(n=n, d=d, r=r):
            p_copy(n, d, r).start()

    slots[far, gy] = joined[...]
    canvas[...] = jnp.zeros(canvas.shape, f32)
    for d in sorted({d for d, _ in peers}, key=abs):

        @pl.when(True if d == 0 else exists(gx, nx, -d))
        def _(d=d):
            for n, (e, r) in enumerate(peers):
                if e == d:
                    p_copy(n, d, r).wait_recv()
            _, there, size = shared(d)
            for b in range(ny):
                spot = (slice(there, there + size), slice(by * b, by * b + by + 4))
                canvas[spot] = canvas[spot] + slots[far + d, b, there : there + size]

    tall = canvas.shape[1]
    shape = (wx, tall, cz)
    point_c, point_k = lane_groups(iota(shape, 2), 6, wz)
    global_i = bx * gx - 2 + iota(shape, 0)
    global_k = bz * gz - 2 + point_k
    row = iota(shape, 1)
    inside = (point_c < 6) & (global_i >= 0) & (global_i < bx * nx)
    inside = inside & (global_k >= 0) & (global_k < bz * nz)
    inside = inside & (row >= 2) & (row < 2 + ly)
    canvas[...] = jnp.where(inside, canvas[...], 0.0)
    own_ref[...] = canvas[2 : 2 + bx]
    window = canvas[:, 0 : by + 4]
    for b in range(1, ny):
        window = jnp.where(gy == b, canvas[:, by * b : by * b + by + 4], window)
    w_ref[...] = window

    for n, o in enumerate(offsets):

        @pl.when(valid(o))
        def _(n=n, o=o):
            halo_copy(n, o).wait_send()

    for n in range(2):

        @pl.when(exists(gz, nz, 1 - 2 * n))
        def _(n=n):
            z_copy(n).wait_send()

    for n, (d, r) in enumerate(peers):

        @pl.when(True if d == 0 else exists(gx, nx, d))
        def _(n=n, d=d, r=r):
            p_copy(n, d, r).wait_send()


def plane_peers(counts, bx):
    nx, ny, _ = counts
    far = min(nx - 1, (bx + 3) // bx)
    pairs = [(d, r) for d in range(-far, far + 1) for r in range(ny)]
    return [pair for pair in pairs if pair != (0, 0)]


def field_kernel(w_ref, own_ref, nv_ref, out_hbm, spread, held, done):
    cx, cy, cz = held.shape[1:]
    ly = nv_ref.shape[3]
    bx, by, bz = cx // 8, cy // 8, cz // 8
    wx, wz = bx + 4, bz + 4
    wy = by + 4
    f32 = jnp.float32
    row = iota((cz, cz), 0)
    group, place = lane_groups(row, 6, wz)
    table = beta(((iota((cz, cz), 1) - 8 * (place - 2)).astype(f32) - 3.5) / 8.0)
    flat = w_ref[...].reshape(wx * wy, cz)
    lane_c, _ = lane_groups(iota((wx * wy, cz), 1), 6, wz)
    stack = jnp.concatenate([jnp.where(lane_c == c, flat, 0.0) for c in range(6)], axis=0)
    spread[...] = dot_split(stack, table).reshape(6, wx, wy, cz)
    sub = (iota((8, cz), 0).astype(f32) - 3.5) / 8.0
    taps = [beta(2.0 - t + sub) for t in range(5)]
    for c in range(6):
        for b in range(by):
            lines = []
            for i in range(wx):
                total = None
                for t in range(5):
                    term = taps[t] * spread[c, i, b + t : b + t + 1]
                    total = term if total is None else total + term
                lines.append(total)
            for x in range(cx):
                block, s = x // 8, x % 8
                half = s // 4
                total = None
                for t in range(half, half + 4):
                    term = beta_static(2 - t + (s - 3.5) / 8.0) * lines[block + t]
                    total = term if total is None else total + term
                held[c, x, 8 * b : 8 * b + 8] = total.astype(jnp.bfloat16)
        pltpu.make_async_copy(held.at[c], out_hbm.at[c // 3, c % 3], done.at[c]).start()
    for i in range(bx):
        for c in range(6):
            moved = own_ref[i]
            moved = pltpu.roll(moved, cz - (c * wz + 2), 1)
            nv_ref[c // 3, c % 3, i] = moved[2 : 2 + ly, 0:bz]
    for c in range(6):
        pltpu.make_async_copy(held.at[c], out_hbm.at[c // 3, c % 3], done.at[c]).wait()


def shards(counts, images, velocity):
    nx, ny, nz = counts
    _, cx, cy, cz = images.shape
    bx, by, bz = cx // 8, cy // 8, cz // 8
    wy = by + 4
    tall = -(-(by * ny + 4) // 8) * 8
    rows = cy + 16
    f32 = jnp.float32
    vmem = pl.BlockSpec(memory_space=pltpu.VMEM)
    hbm = pl.BlockSpec(memory_space=pl.ANY)
    offsets = 26
    peers = plane_peers(counts, bx)
    far = max(d for d, _ in peers)
    wx = bx + 4
    window, own = pl.pallas_call(
        functools.partial(force_kernel, counts, (cx, cy, cz)),
        out_shape=(
            pltpu.VMEM((wx, wy, cz), f32),
            pltpu.VMEM((bx, tall, cz), f32),
        ),
        in_specs=[hbm, hbm],
        out_specs=(vmem, vmem),
        scratch_shapes=[
            pltpu.VMEM((2, cx + 2 * RAD, rows, cz), f32),
            pltpu.VMEM(velocity.shape, f32),
            pltpu.VMEM((2, 3, rows, cz), f32),
            pltpu.VMEM((2, cy, cz), f32),
            pltpu.VMEM((20, rows, cz), f32),
            pltpu.VMEM((20, cy + 8, cz), f32),
            pltpu.VMEM((6, cy, cz), f32),
            pltpu.VMEM((6, wx, cy, cz), f32),
            pltpu.VMEM((bx, wy, cz), f32),
            pltpu.VMEM((wx, wy, cz), f32),
            pltpu.VMEM((wx, wy, cz), f32),
            pltpu.VMEM((2, wx, wy, cz), f32),
            pltpu.VMEM((2 * far + 1, ny, wx, wy, cz), f32),
            pltpu.VMEM((wx, tall, cz), f32),
            pltpu.SemaphoreType.DMA((2,)),
            pltpu.SemaphoreType.DMA((offsets,)),
            pltpu.SemaphoreType.DMA((offsets,)),
            pltpu.SemaphoreType.DMA((2,)),
            pltpu.SemaphoreType.DMA((2,)),
            pltpu.SemaphoreType.DMA((len(peers),)),
            pltpu.SemaphoreType.DMA((len(peers),)),
        ],
        compiler_params=pltpu.CompilerParams(collective_id=0, has_side_effects=True),
        name="forces",
    )(images, velocity)
    new_velocity, field = pl.pallas_call(
        field_kernel,
        out_shape=(
            jax.ShapeDtypeStruct(velocity.shape, f32),
            jax.ShapeDtypeStruct((2, 3, cx, cy, cz), jnp.bfloat16),
        ),
        in_specs=[vmem, vmem],
        out_specs=(vmem, hbm),
        scratch_shapes=[
            pltpu.VMEM((6, wx, wy, cz), f32),
            pltpu.VMEM((6, cx, cy, cz), jnp.bfloat16),
            pltpu.SemaphoreType.DMA((6,)),
        ],
        name="field",
    )(
        pltpu.with_memory_space_constraint(window, pltpu.VMEM),
        pltpu.with_memory_space_constraint(own, pltpu.VMEM),
    )
    return new_velocity, field


def solution(mesh):
    placed = (P(None, "gx", "gy", "gz"), P(None, None, "gx", None, "gz"))
    counts = tuple(mesh.shape[a] for a in ("gx", "gy", "gz"))
    return jax.shard_map(
        functools.partial(shards, counts),
        mesh=mesh,
        in_specs=placed,
        out_specs=(P(None, None, "gx", None, "gz"), P(None, None, "gx", "gy", "gz")),
        check_vma=False,
    )
```
